32 devices in a mesh: ep: 4 (over y, x), tp: 8 (over z, core).
Axes of the slice: x: 2, y: 2, z: 4, core: 2. Of those that a mesh axis runs over, the one named last changes fastest.
Arguments:
- tokens: bfloat16 [512, 6144], P('ep'), may hold values from -6 to 6
- expert_ids: int32 [512, 2], P('ep'), may hold values from 0 to 3, all different within a row; in each aligned block of 128 rows (0 to 127, 128 to 255, ...) at most 96 rows name the same one
- router: bfloat16 [6144, 4], replicated, may hold values from -0.078125 to 0.078125
- gate_weight: bfloat16 [4, 6144, 8192], P('ep', None, 'tp'), may hold values from -0.078125 to 0.078125
- up_weight: bfloat16 [4, 6144, 8192], P('ep', None, 'tp'), may hold values from -0.078125 to 0.078125
- down_weight: bfloat16 [4, 8192, 6144], P('ep', 'tp'), may hold values from -0.0625 to 0.0625
- keep_mask: int32 [512, 6144], P('ep'), may hold values 0 or 1
Outputs:
- layer_out: bfloat16 [512, 6144], P('ep')
The draws below stay inside these ranges and needn't reach their ends.
Inputs may be any that keep to these rules, and one draw needn't show every extreme that they name: `expert_ids`: each row names two different experts. In the rows of one token block of 128 rows no expert is named more than 96 times, a bound that some block reaches.
All inputs are finite; a program needn't handle non-finite values. No bound on the sum of `keep_mask` on one device may be relied on, other than what follows from the above.
Results may differ from the reference program's by a relative error of at most 0.018.
Values may be sent and summed in bfloat16 or wider, within the bound.
A program may use at most 128 MiB of HBM per device.

```python
import math
import jax
import jax.numpy as jnp
import numpy as np
from jax import lax

D = 6144
FF = 8192
TOK_DEV = 128
EXPERTS = 4
CAP = 96
TOKENS = 512
N_EP = 4
N_TP = 8


def set_ends(drawn, rng, smallest, top_value):
    index_at = [jax.random.randint(jax.random.fold_in(rng, axis), (), 0, length) for axis, length in enumerate(drawn.shape)]
    longest = drawn.shape.index(max(drawn.shape))
    next_to = index_at[:longest] + [(index_at[longest] + 1) % drawn.shape[longest]] + index_at[longest + 1:]
    return drawn.at[tuple(index_at)].set(smallest).at[tuple(next_to)].set(top_value)


def levels(key, extent, pieces, least, largest):
    def one(dim, shards_of):
        steps = jax.random.uniform(jax.random.fold_in(jax.random.fold_in(key, 6), dim), (shards_of,), jnp.float32, least / len(pieces), largest / len(pieces))
        return jnp.repeat(jnp.exp(steps), extent[dim] // shards_of).reshape((-1,) + (1,) * (len(extent) - dim - 1))

    gain = one(*pieces[0])
    for cut in pieces[1:]:
        gain = gain * one(*cut)
    return gain


def assign_block(key, own, number, rows, count, top, limit, skew):
    ranking = jax.random.permutation(key, count)
    heavy_load, ordinary = shares(count, rows * top, limit, skew, True), shares(count, rows * top, limit, skew, False)
    places = jnp.arange(count)

    def named(tallies, offset_by):
        used = int((tallies > 0).sum())
        fixed = max(1, used // 4)
        moved = fixed + (places - fixed + offset_by * (used - fixed)) % max(1, count - fixed)
        return jnp.zeros((count,), jnp.int32).at[ranking[jnp.where(places < fixed, places, moved)]].set(jnp.asarray(tallies, jnp.int32))

    tallies = jnp.where(number % 4 == 0, named(heavy_load, number // 4), named(ordinary, number - number // 4 - 1))
    mixed = jax.random.permutation(jax.random.fold_in(own, 3), count)
    source_of, receiver = mixed[0:count // 2 * 2:2], mixed[1:count // 2 * 2:2]
    slack = jnp.minimum(tallies[source_of] - 1, limit - tallies[receiver]) // 2
    slack = jnp.where((source_of == ranking[0]) | (receiver == ranking[0]) | (tallies[receiver] == 0), 0, jnp.maximum(slack, 0))
    moved = jax.random.randint(jax.random.fold_in(own, 4), (count // 2,), 0, 1 << 20) % (slack + 1)
    tallies = tallies.at[source_of].add(-moved).at[receiver].add(moved)
    labels = jnp.searchsorted(jnp.cumsum(tallies), jnp.arange(rows * top), side="right").astype(jnp.int32)
    listing = labels.reshape(top, rows).T
    listing = listing[jax.random.permutation(jax.random.fold_in(own, 1), rows)]
    offset_by = jax.random.randint(jax.random.fold_in(own, 2), (rows, 1), 0, top)
    return jnp.take_along_axis(listing, (jnp.arange(top)[None, :] + offset_by) % top, axis=1)


def shares(count, total, bound, slope, full):
    weights = [(1 << 20) // math.isqrt(rank ** slope) + 1 for rank in range(1, count + 1)]
    largest = bound if full else min(bound, max(-(-total // count), total * weights[0] // sum(weights)))
    least = 1 if total - largest >= count - 1 else 0
    holding, rest = [largest] + [least] * (count - 1), total - largest - least * (count - 1)
    while rest > 0:
        movable = [i for i in range(1, count) if holding[i] < largest] or [i for i in range(1, count) if holding[i] < bound]
        mass, budget = sum([weights[i] for i in movable]), rest
        for i in movable:
            more = min(bound - holding[i], max(1, budget * weights[i] // mass), rest)
            holding[i] = holding[i] + more
            rest = rest - more
    return np.array(holding)


def centred(own_key, extent, spread, limit, split=(), kind=jnp.bfloat16):
    values = jax.random.normal(own_key, extent, jnp.float32) * spread
    if len(split) > 0:
        values = levels(own_key, extent, split, -0.22, 0.18) * values
    return jnp.clip(values, min=-limit, max=limit).astype(kind)


def setup_inputs(seed: int = 0) -> dict:
    splits = jax.random.split(jax.random.key(seed), 8)
    tokens = centred(splits[0], (TOKENS, D), 1.0, 6.0, ((0, 4),))
    expert_ids_keys = jax.random.split(jax.random.fold_in(splits[1], 1), TOKENS // TOK_DEV)
    expert_ids_turns = jax.random.permutation(jax.random.fold_in(splits[1], 3), TOKENS // TOK_DEV)
    expert_ids = jax.vmap(lambda own, number: assign_block(jax.random.fold_in(splits[1], 2), own, number, TOK_DEV, EXPERTS, 2, CAP, 2))(expert_ids_keys, expert_ids_turns).reshape((TOKENS, 2))
    router = centred(splits[2], (D, EXPERTS), D ** -0.5, 0.078125)
    gate_weight = centred(splits[3], (EXPERTS, D, FF), D ** -0.5, 0.078125, ((0, 4), (2, 8)))
    up_weight = centred(splits[4], (EXPERTS, D, FF), D ** -0.5, 0.078125, ((0, 4), (2, 8)))
    down_weight = centred(splits[5], (EXPERTS, FF, D), FF ** -0.5, 0.0625, ((0, 4), (1, 8)))
    keep_mask = set_ends((jax.random.randint(splits[6], (TOKENS, D), 0, 5) < 4).astype(jnp.int32), jax.random.fold_in(splits[6], 1), 0, 1)
    return dict(tokens=tokens, expert_ids=expert_ids, router=router, gate_weight=gate_weight, up_weight=up_weight, down_weight=down_weight, keep_mask=keep_mask)


def reference(tokens, expert_ids, router, gate_weight, up_weight, down_weight, keep_mask):
    total_rows = tokens.shape[0]
    logits = jnp.dot(tokens, router, preferred_element_type=jnp.float32)
    picked = jnp.take_along_axis(logits, expert_ids, axis=1)
    weight_first = jax.nn.sigmoid(picked[:, 0] - picked[:, 1])
    weight_second = jax.nn.sigmoid(picked[:, 1] - picked[:, 0])
    onehot = (expert_ids[:, :, None] == jnp.arange(EXPERTS, dtype=jnp.int32)[None, None, :]).astype(jnp.int32)
    blocked = onehot.reshape(N_EP, TOK_DEV * 2, EXPERTS)
    ranks = jnp.cumsum(blocked, axis=1) - blocked
    slot = jnp.sum(ranks * blocked, axis=2).reshape(total_rows, 2)
    block_of = jnp.arange(total_rows, dtype=jnp.int32) // TOK_DEV
    place = (block_of[:, None] * CAP + slot).astype(jnp.int32)
    token_index = jnp.broadcast_to(jnp.arange(total_rows, dtype=jnp.int32)[:, None], (total_rows, 2))
    table = jnp.full((EXPERTS, N_EP * CAP), total_rows, jnp.int32)
    table = table.at[expert_ids, place].set(token_index)
    padded = jnp.concatenate([tokens, jnp.zeros((1, tokens.shape[1]), jnp.bfloat16)], axis=0)
    width = FF // N_TP

    def one_expert(inputs):
        w_gate, w_up, w_down, rows_index = inputs
        buffer = jnp.take(padded, rows_index, axis=0)
        gate = jnp.dot(buffer, w_gate, preferred_element_type=jnp.float32)
        up = jnp.dot(buffer, w_up, preferred_element_type=jnp.float32)
        hidden = (jax.nn.silu(gate) * up).astype(jnp.bfloat16)

        def add_block(block, total):
            start = (block * width).astype(jnp.int32)
            h_block = lax.dynamic_slice_in_dim(hidden, start, width, 1)
            d_block = lax.dynamic_slice_in_dim(w_down, start, width, 0)
            partial_sum = jnp.dot(h_block, d_block, preferred_element_type=jnp.float32)
            rounded = lax.optimization_barrier(partial_sum.astype(jnp.bfloat16))
            return total + rounded.astype(jnp.float32)

        empty = jnp.zeros((buffer.shape[0], buffer.shape[1]), jnp.float32)
        summed = lax.fori_loop(0, N_TP, add_block, empty)
        return summed.astype(jnp.bfloat16)

    outputs = lax.map(one_expert, (gate_weight, up_weight, down_weight, table))
    first_rows = outputs[expert_ids[:, 0], place[:, 0]].astype(jnp.float32)
    second_rows = outputs[expert_ids[:, 1], place[:, 1]].astype(jnp.float32)
    combined = weight_first[:, None] * first_rows + weight_second[:, None] * second_rows
    return (combined * keep_mask.astype(jnp.float32) * 1.25).astype(jnp.bfloat16)
```

```python
import functools

import jax
import jax.numpy as jnp
from jax import lax
from jax.experimental import pallas as pl
from jax.experimental.pallas import tpu as pltpu
from jax.sharding import PartitionSpec as P

MESH = pl.DeviceIdType.MESH


def flip(index, offset, count):
    out, bit = 0, 1
    while bit < count:
        out = out + ((index // bit + offset // bit) % 2) * bit
        bit *= 2
    return out


def kernel(
    n_ep, nz, slots_ref, comb_ref, gate_hbm, up_hbm, down_hbm, mask_hbm, out_ref,
    w_gate, w_up, w_down, mask, rows, hidden, pair_out, pair_in, mine, ep_out, ep_in,
    z_out, z_in, local_sem, disp_s, disp_r, fwd_s, fwd_r, pair_s, pair_r, ep_s, ep_r,
    z_s, z_r, gat_s, gat_r, gfw_s, gfw_r,
):
    ep, tp = lax.axis_index("ep"), lax.axis_index("tp")
    z, core = tp // 2, tp % 2
    partner = (ep, z * 2 + (1 - core))
    cap, width = rows.shape[1], rows.shape[2]
    toks = out_ref.shape[0]
    ff = w_gate.shape[1]
    half, piece = width // 2, width // (2 * nz)
    total_rows = n_ep * cap

    def cols(owner_core, owner_z):
        return pl.ds(pl.multiple_of((owner_core * nz + owner_z) * piece, 128), piece)

    my_half = pl.ds(pl.multiple_of(core * half, 128), half)

    load_own = pltpu.make_async_copy(slots_ref.at[ep], rows.at[0], local_sem.at[0])
    load_gate = pltpu.make_async_copy(gate_hbm, w_gate, local_sem.at[1])
    load_up = pltpu.make_async_copy(up_hbm, w_up, local_sem.at[2])
    load_down = pltpu.make_async_copy(down_hbm, w_down, local_sem.at[3])
    load_mask = pltpu.make_async_copy(mask_hbm.at[:, cols(core, z)], mask, local_sem.at[4])
    for load in (load_own, load_gate, load_up):
        load.start()

    barrier = pltpu.get_barrier_semaphore()
    peers = [(flip(ep, o, n_ep), tp) for o in range(1, n_ep)]
    peers += [(ep, ((z + s) % nz) * 2 + core) for s in range(1, nz)] + [partner]
    for peer in peers:
        pl.semaphore_signal(barrier, inc=1, device_id=peer, device_id_type=MESH)
    pl.semaphore_wait(barrier, len(peers))

    def remote(src, dst, send, recv, device):
        return pltpu.make_async_remote_copy(
            src_ref=src, dst_ref=dst, send_sem=send, recv_sem=recv,
            device_id=device, device_id_type=MESH,
        )

    started = []

    dispatch = [None]
    for o in range(1, n_ep):
        peer = flip(ep, o, n_ep)
        copy = remote(slots_ref.at[peer, :, my_half], rows.at[o, :, my_half],
                      disp_s.at[o], disp_r.at[o], (peer, tp))
        copy.start()
        dispatch.append(copy)
        started.append(copy)
    load_down.start()
    load_mask.start()

    forward = [None]
    for o in range(1, n_ep):
        forward.append(remote(rows.at[o, :, my_half], rows.at[o, :, my_half],
                              fwd_s.at[o], fwd_r.at[o], partner))

    tile = min(256, ff)
    phases = 2
    per = n_ep // phases
    for phase in range(phases):
        for o in range(phase * per, (phase + 1) * per):
            if o > 0:
                dispatch[o].wait_recv()
                forward[o].start()
                started.append(forward[o])
        if phase == 0:
            load_own.wait()
            load_gate.wait()
            load_up.wait()
        for o in range(phase * per, (phase + 1) * per):
            if o > 0:
                forward[o].wait_recv()

        def up_step(t, carry):
            at = pl.ds(pl.multiple_of(t * tile, tile), tile)
            block = rows[phase * per:(phase + 1) * per].reshape(per * cap, width)
            gate = jnp.dot(block, w_gate[:, at], preferred_element_type=jnp.float32)
            up = jnp.dot(block, w_up[:, at], preferred_element_type=jnp.float32)
            hidden[phase * per * cap:(phase + 1) * per * cap, at] = (
                jax.nn.silu(gate) * up).astype(jnp.bfloat16)
            return carry

        lax.fori_loop(0, ff // tile, up_step, 0)

    load_down.wait()

    def pair_sum(s):
        pair[s].wait_recv()
        summed = (mine[s % 2].astype(jnp.float32) + pair_in[s].astype(jnp.float32)).astype(jnp.bfloat16)
        ep_in[s, 0:cap, :] = summed[0:cap]
        ep_out[s] = summed[cap:]
        for o in range(1, n_ep):
            copy = remote(ep_out.at[s, pl.ds((o - 1) * cap, cap), :], ep_in.at[s, pl.ds(o * cap, cap), :],
                          ep_s.at[s, o], ep_r.at[s, o], (flip(ep, o, n_ep), tp))
            copy.start()
            exchange[s].append(copy)
            started.append(copy)

    pair, exchange = [], [[] for _ in range(nz)]
    for s in range(nz):
        owner = (z + 1 + s) % nz
        pair_out[s] = jnp.dot(hidden[...], w_down[:, cols(1 - core, owner)],
                              preferred_element_type=jnp.float32).astype(jnp.bfloat16)
        copy = remote(pair_out.at[s], pair_in.at[s], pair_s.at[s], pair_r.at[s], partner)
        copy.start()
        pair.append(copy)
        started.append(copy)
        mine[s % 2] = jnp.dot(hidden[...], w_down[:, cols(core, owner)],
                              preferred_element_type=jnp.float32).astype(jnp.bfloat16)
        pair_sum(s)

    reduce = []
    for s in range(nz):
        owner = (z + 1 + s) % nz
        for copy in exchange[s]:
            copy.wait_recv()
        both = jnp.dot(comb_ref[...], ep_in[s], preferred_element_type=jnp.float32)
        token_sum = both[0:toks] + both[toks:]
        if s < nz - 1:
            z_out[s] = token_sum.astype(jnp.bfloat16)
            copy = remote(z_out.at[s], z_in.at[s], z_s.at[s], z_r.at[s], (ep, owner * 2 + core))
            copy.start()
            reduce.append(copy)
            started.append(copy)
    for s in range(nz - 1):
        reduce[s].wait_recv()
        token_sum = token_sum + z_in[s].astype(jnp.float32)
    load_mask.wait()
    out_ref[:, cols(core, z)] = (token_sum * mask[...].astype(jnp.float32) * 1.25).astype(jnp.bfloat16)

    gather = []
    here = out_ref.at[:, cols(core, z)]
    for s in range(1, nz):
        copy = remote(here, here, gat_s.at[s], gat_r.at[s], (ep, ((z + s) % nz) * 2 + core))
        copy.start()
        gather.append(copy)
        started.append(copy)
    passed = [remote(here, here, gfw_s.at[0], gfw_r.at[0], partner)]
    passed[0].start()
    started.append(passed[0])
    for s in range(1, nz):
        gather[s - 1].wait_recv()
        there = out_ref.at[:, cols(core, (z + nz - s) % nz)]
        copy = remote(there, there, gfw_s.at[s], gfw_r.at[s], partner)
        copy.start()
        passed.append(copy)
        started.append(copy)
    for copy in passed:
        copy.wait_recv()
    for copy in started:
        copy.wait_send()


def shards(n_ep, n_tp, tokens, expert_ids, router, gate_weight, up_weight, down_weight, keep_mask):
    experts = router.shape[1]
    toks, width = tokens.shape
    cap = 3 * toks // experts
    nz = n_tp // 2
    piece = width // n_tp
    total = experts * cap
    logits = jnp.dot(tokens, router, preferred_element_type=jnp.float32)
    numbers = jnp.arange(experts, dtype=jnp.int32)
    onehot3 = expert_ids[:, :, None] == numbers[None, None, :]
    picked = jnp.sum(jnp.where(onehot3, logits[:, None, :], 0.0), axis=2)
    weight_first = jax.nn.sigmoid(picked[:, 0] - picked[:, 1])
    weight_second = jax.nn.sigmoid(picked[:, 1] - picked[:, 0])
    onehot = onehot3.astype(jnp.float32)
    named = onehot[:, 0] + onehot[:, 1]
    order = jnp.arange(toks, dtype=jnp.int32)
    before = (order[None, :] < order[:, None]).astype(jnp.bfloat16)
    ranks = jnp.dot(before, named.astype(jnp.bfloat16), preferred_element_type=jnp.float32)
    slot = jnp.sum(ranks[:, None, :] * onehot, axis=2).astype(jnp.int32)
    lines = jnp.arange(total, dtype=jnp.int32)
    place = expert_ids * cap + slot
    picker = ((place[None, :, 0] == lines[:, None]) | (place[None, :, 1] == lines[:, None])).astype(jnp.bfloat16)
    slots = jnp.dot(picker, tokens, preferred_element_type=jnp.float32).astype(jnp.bfloat16)
    slots = slots.reshape(experts, cap, width)
    turned = jnp.bitwise_xor(expert_ids, lax.axis_index("ep")) * cap + slot
    comb = (jnp.where(turned[:, 0:1] == lines[None, :], weight_first[:, None], 0.0)
            + jnp.where(turned[:, 1:2] == lines[None, :], weight_second[:, None], 0.0))
    high = lax.reduce_precision(comb, 8, 7)
    comb = jnp.concatenate([high, comb - high], axis=0).astype(jnp.bfloat16)
    w_gate, w_up, w_down = gate_weight[0], up_weight[0], down_weight[0]
    ff = w_gate.shape[1]
    vmem, hbm = pl.BlockSpec(memory_space=pltpu.VMEM), pl.BlockSpec(memory_space=pl.ANY)
    bf = jnp.bfloat16
    dma = pltpu.SemaphoreType.DMA
    return pl.pallas_call(
        functools.partial(kernel, n_ep, nz),
        out_shape=jax.ShapeDtypeStruct((toks, width), bf),
        in_specs=[vmem, vmem, hbm, hbm, hbm, hbm],
        out_specs=vmem,
        scratch_shapes=[
            pltpu.VMEM((width, ff), bf), pltpu.VMEM((width, ff), bf), pltpu.VMEM((ff, width), bf),
            pltpu.VMEM((toks, piece), jnp.int32),
            pltpu.VMEM((experts, cap, width), bf),
            pltpu.VMEM((total, ff), bf),
            pltpu.VMEM((nz, total, piece), bf), pltpu.VMEM((nz, total, piece), bf),
            pltpu.VMEM((2, total, piece), bf),
            pltpu.VMEM((nz, total - cap, piece), bf), pltpu.VMEM((nz, total, piece), bf),
            pltpu.VMEM((nz - 1, toks, piece), bf), pltpu.VMEM((nz - 1, toks, piece), bf),
            dma((5,)), dma((n_ep,)), dma((n_ep,)), dma((n_ep,)), dma((n_ep,)),
            dma((nz,)), dma((nz,)), dma((nz, n_ep)), dma((nz, n_ep)),
            dma((nz,)), dma((nz,)), dma((nz,)), dma((nz,)), dma((nz,)), dma((nz,)),
        ],
        compiler_params=pltpu.CompilerParams(
            collective_id=0, has_side_effects=True, vmem_limit_bytes=67043328),
    )(slots, comb, w_gate, w_up, w_down, keep_mask)


def solution(mesh):
    return jax.shard_map(
        functools.partial(shards, mesh.shape["ep"], mesh.shape["tp"]),
        mesh=mesh,
        in_specs=(
            P("ep", None),
            P("ep", None),
            P(),
            P("ep", None, "tp"),
            P("ep", None, "tp"),
            P("ep", "tp", None),
            P("ep", None),
        ),
        out_specs=P("ep", None),
        check_vma=False,
    )
```

```python
import functools

import jax
import jax.numpy as jnp
from jax import lax
from jax.experimental import pallas as pl
from jax.experimental.pallas import tpu as pltpu
from jax.sharding import PartitionSpec as P

MESH = pl.DeviceIdType.MESH


def flip(index, offset, count):
    out, bit = 0, 1
    while bit < count:
        out = out + ((index // bit + offset // bit) % 2) * bit
        bit *= 2
    return out


def kernel(
    n_ep, nz, slots_ref, comb_ref, gate_hbm, up_hbm, down_hbm, mask_hbm, out_ref,
    w_gate, w_up, w_down, mask, rows, hidden, pair_out, pair_in, mine, ep_out, ep_in,
    z_out, z_in, local_sem, disp_s, disp_r, fwd_s, fwd_r, pair_s, pair_r, ep_s, ep_r,
    z_s, z_r, gat_s, gat_r, gfw_s, gfw_r,
):
    ep, tp = lax.axis_index("ep"), lax.axis_index("tp")
    z, core = tp // 2, tp % 2
    partner = (ep, z * 2 + (1 - core))
    cap, width = rows.shape[1], rows.shape[2]
    toks = out_ref.shape[0]
    ff = w_gate.shape[1]
    half, piece = width // 2, width // (2 * nz)
    total_rows = n_ep * cap

    rounds = pair_in.shape[0] // nz
    sub = piece // rounds

    def cols(owner_core, owner_z, turn=None):
        if turn is None:
            return pl.ds(pl.multiple_of((owner_core * nz + owner_z) * piece, 128), piece)
        return pl.ds(pl.multiple_of((owner_core * nz + owner_z) * piece + turn * sub, 128), sub)

    my_half = pl.ds(pl.multiple_of(core * half, 128), half)

    load_own = pltpu.make_async_copy(slots_ref.at[ep], rows.at[0], local_sem.at[0])
    load_gate = pltpu.make_async_copy(gate_hbm, w_gate, local_sem.at[1])
    load_up = pltpu.make_async_copy(up_hbm, w_up, local_sem.at[2])
    load_down = pltpu.make_async_copy(down_hbm, w_down, local_sem.at[3])
    load_mask = pltpu.make_async_copy(mask_hbm.at[:, cols(core, z)], mask, local_sem.at[4])
    for load in (load_own, load_gate, load_up):
        load.start()

    barrier = pltpu.get_barrier_semaphore()
    peers = [(flip(ep, o, n_ep), tp) for o in range(1, n_ep)]
    peers += [(ep, ((z + s) % nz) * 2 + core) for s in range(1, nz)] + [partner]
    for peer in peers:
        pl.semaphore_signal(barrier, inc=1, device_id=peer, device_id_type=MESH)
    pl.semaphore_wait(barrier, len(peers))

    def remote(src, dst, send, recv, device):
        return pltpu.make_async_remote_copy(
            src_ref=src, dst_ref=dst, send_sem=send, recv_sem=recv,
            device_id=device, device_id_type=MESH,
        )

    started = []

    third = half // 3
    odd = z % 2
    z_pair = (ep, (z + 1 - 2 * odd) * 2 + core)

    def part(which):
        return pl.ds(pl.multiple_of(core * half + which * third, 128), third)

    shared, common, foreign = part(2 * odd), part(1), part(2 - 2 * odd)
    arrive, forward = {}, {}

    def send_rows(o, kind, at):
        peer = flip(ep, o, n_ep)
        copy = remote(slots_ref.at[peer, :, at], rows.at[o, :, at],
                      disp_s.at[kind, o], disp_r.at[kind, o], (peer, tp))
        copy.start()
        arrive[kind, o] = copy
        started.append(copy)

    def pass_on(o, kind, at):
        arrive[kind, o].wait_recv()
        if kind == 0:
            copy = remote(rows.at[o, :, at], rows.at[o, :, at],
                          disp_s.at[2, o], disp_r.at[2, o], z_pair)
            copy.start()
            arrive[2, o] = copy
            started.append(copy)
        copy = remote(rows.at[o, :, at], rows.at[o, :, at],
                      fwd_s.at[kind, o], fwd_r.at[kind, o], partner)
        copy.start()
        forward[kind, o] = copy
        started.append(copy)

    share_order = [n_ep - 1] + list(range(1, n_ep - 1))
    for o in share_order:
        send_rows(o, 0, shared)
    for o in range(1, n_ep):
        send_rows(o, 1, common)
    load_down.start()
    load_mask.start()
    for o in share_order:
        pass_on(o, 0, shared)

    tile = min(256, ff)
    phases = 2
    per = n_ep // phases
    for phase in range(phases):
        for o in range(phase * per, (phase + 1) * per):
            if o > 0:
                pass_on(o, 1, common)
                pass_on(o, 2, foreign)
        if phase == 0:
            load_own.wait()
            load_gate.wait()
            load_up.wait()
        for o in range(phase * per, (phase + 1) * per):
            if o > 0:
                for kind in range(3):
                    forward[kind, o].wait_recv()

        def up_step(t, carry):
            at = pl.ds(pl.multiple_of(t * tile, tile), tile)
            block = rows[phase * per:(phase + 1) * per].reshape(per * cap, width)
            gate = jnp.dot(block, w_gate[:, at], preferred_element_type=jnp.float32)
            up = jnp.dot(block, w_up[:, at], preferred_element_type=jnp.float32)
            hidden[phase * per * cap:(phase + 1) * per * cap, at] = (
                jax.nn.silu(gate) * up).astype(jnp.bfloat16)
            return carry

        lax.fori_loop(0, ff // tile, up_step, 0)

    load_down.wait()

    def pair_sum(s):
        pair[s].wait_recv()
        summed = (mine[s % 2].astype(jnp.float32) + pair_in[s].astype(jnp.float32)).astype(jnp.bfloat16)
        ep_in[s, 0:cap, :] = summed[0:cap]
        ep_out[s] = summed[cap:]
        for o in range(1, n_ep):
            copy = remote(ep_out.at[s, pl.ds((o - 1) * cap, cap), :], ep_in.at[s, pl.ds(o * cap, cap), :],
                          ep_s.at[s, o], ep_r.at[s, o], (flip(ep, o, n_ep), tp))
            copy.start()
            exchange[s].append(copy)
            started.append(copy)

    pair, exchange = [], [[] for _ in range(rounds * nz)]
    for s in range(rounds * nz):
        turn, owner = s // nz, (z + 1 + s % nz) % nz
        pair_out[s] = jnp.dot(hidden[...], w_down[:, cols(1 - core, owner, turn)],
                              preferred_element_type=jnp.float32).astype(jnp.bfloat16)
        copy = remote(pair_out.at[s], pair_in.at[s], pair_s.at[s], pair_r.at[s], partner)
        copy.start()
        pair.append(copy)
        started.append(copy)
        if s > 0:
            pair_sum(s - 1)
        mine[s % 2] = jnp.dot(hidden[...], w_down[:, cols(core, owner, turn)],
                              preferred_element_type=jnp.float32).astype(jnp.bfloat16)
    pair_sum(rounds * nz - 1)

    load_mask.wait()
    gather = {}
    passed = []

    def hand_over(turn):
        for s in range(1, nz):
            gather[turn, s].wait_recv()
            there = out_ref.at[:, cols(core, (z + nz - s) % nz, turn)]
            copy = remote(there, there, gfw_s.at[turn, s], gfw_r.at[turn, s], partner)
            copy.start()
            passed.append(copy)
            started.append(copy)

    for turn in range(rounds):
        reduce = []
        for s in range(nz):
            step = turn * nz + s
            owner = (z + 1 + s) % nz
            for copy in exchange[step]:
                copy.wait_recv()
            both = jnp.dot(comb_ref[...], ep_in[step], preferred_element_type=jnp.float32)
            token_sum = both[0:toks] + both[toks:]
            if s < nz - 1:
                z_out[turn, s] = token_sum.astype(jnp.bfloat16)
                copy = remote(z_out.at[turn, s], z_in.at[turn, s], z_s.at[turn, s], z_r.at[turn, s],
                              (ep, owner * 2 + core))
                copy.start()
                reduce.append(copy)
                started.append(copy)
        for s in range(nz - 1):
            reduce[s].wait_recv()
            token_sum = token_sum + z_in[turn, s].astype(jnp.float32)
        keep = mask[:, turn * sub:(turn + 1) * sub].astype(jnp.float32)
        out_ref[:, cols(core, z, turn)] = (token_sum * keep * 1.25).astype(jnp.bfloat16)
        here = out_ref.at[:, cols(core, z, turn)]
        for s in range(1, nz):
            copy = remote(here, here, gat_s.at[turn, s], gat_r.at[turn, s], (ep, ((z + s) % nz) * 2 + core))
            copy.start()
            gather[turn, s] = copy
            started.append(copy)
        copy = remote(here, here, gfw_s.at[turn, 0], gfw_r.at[turn, 0], partner)
        copy.start()
        passed.append(copy)
        started.append(copy)
        if turn > 0:
            hand_over(turn - 1)
    hand_over(rounds - 1)
    for copy in passed:
        copy.wait_recv()
    for copy in started:
        copy.wait_send()


def shards(n_ep, n_tp, tokens, expert_ids, router, gate_weight, up_weight, down_weight, keep_mask):
    experts = router.shape[1]
    toks, width = tokens.shape
    cap = 3 * toks // experts
    nz = n_tp // 2
    piece = width // n_tp
    total = experts * cap
    rounds = 3 if piece % 384 == 0 and piece > 384 else 1
    sub, steps = piece // rounds, rounds * nz
    logits = jnp.dot(tokens, router, preferred_element_type=jnp.float32)
    numbers = jnp.arange(experts, dtype=jnp.int32)
    onehot3 = expert_ids[:, :, None] == numbers[None, None, :]
    picked = jnp.sum(jnp.where(onehot3, logits[:, None, :], 0.0), axis=2)
    weight_first = jax.nn.sigmoid(picked[:, 0] - picked[:, 1])
    weight_second = jax.nn.sigmoid(picked[:, 1] - picked[:, 0])
    onehot = onehot3.astype(jnp.float32)
    named = onehot[:, 0] + onehot[:, 1]
    order = jnp.arange(toks, dtype=jnp.int32)
    before = (order[None, :] < order[:, None]).astype(jnp.bfloat16)
    ranks = jnp.dot(before, named.astype(jnp.bfloat16), preferred_element_type=jnp.float32)
    slot = jnp.sum(ranks[:, None, :] * onehot, axis=2).astype(jnp.int32)
    lines = jnp.arange(total, dtype=jnp.int32)
    place = expert_ids * cap + slot
    picker = ((place[None, :, 0] == lines[:, None]) | (place[None, :, 1] == lines[:, None])).astype(jnp.bfloat16)
    slots = jnp.dot(picker, tokens, preferred_element_type=jnp.float32).astype(jnp.bfloat16)
    slots = slots.reshape(experts, cap, width)
    turned = jnp.bitwise_xor(expert_ids, lax.axis_index("ep")) * cap + slot
    comb = (jnp.where(turned[:, 0:1] == lines[None, :], weight_first[:, None], 0.0)
            + jnp.where(turned[:, 1:2] == lines[None, :], weight_second[:, None], 0.0))
    high = lax.reduce_precision(comb, 8, 7)
    comb = jnp.concatenate([high, comb - high], axis=0).astype(jnp.bfloat16)
    w_gate, w_up, w_down = gate_weight[0], up_weight[0], down_weight[0]
    ff = w_gate.shape[1]
    vmem, hbm = pl.BlockSpec(memory_space=pltpu.VMEM), pl.BlockSpec(memory_space=pl.ANY)
    bf = jnp.bfloat16
    dma = pltpu.SemaphoreType.DMA
    return pl.pallas_call(
        functools.partial(kernel, n_ep, nz),
        out_shape=jax.ShapeDtypeStruct((toks, width), bf),
        in_specs=[vmem, vmem, hbm, hbm, hbm, hbm],
        out_specs=vmem,
        scratch_shapes=[
            pltpu.VMEM((width, ff), bf), pltpu.VMEM((width, ff), bf), pltpu.VMEM((ff, width), bf),
            pltpu.VMEM((toks, piece), jnp.int32),
            pltpu.VMEM((experts, cap, width), bf),
            pltpu.VMEM((total, ff), bf),
            pltpu.VMEM((steps, total, sub), bf), pltpu.VMEM((steps, total, sub), bf),
            pltpu.VMEM((2, total, sub), bf),
            pltpu.VMEM((steps, total - cap, sub), bf), pltpu.VMEM((steps, total, sub), bf),
            pltpu.VMEM((rounds, nz - 1, toks, sub), bf), pltpu.VMEM((rounds, nz - 1, toks, sub), bf),
            dma((5,)), dma((3, n_ep)), dma((3, n_ep)), dma((3, n_ep)), dma((3, n_ep)),
            dma((steps,)), dma((steps,)), dma((steps, n_ep)), dma((steps, n_ep)),
            dma((rounds, nz)), dma((rounds, nz)), dma((rounds, nz)), dma((rounds, nz)),
            dma((rounds, nz)), dma((rounds, nz)),
        ],
        compiler_params=pltpu.CompilerParams(
            collective_id=0, has_side_effects=True, vmem_limit_bytes=67043328),
    )(slots, comb, w_gate, w_up, w_down, keep_mask)


def solution(mesh):
    return jax.shard_map(
        functools.partial(shards, mesh.shape["ep"], mesh.shape["tp"]),
        mesh=mesh,
        in_specs=(
            P("ep", None),
            P("ep", None),
            P(),
            P("ep", None, "tp"),
            P("ep", None, "tp"),
            P("ep", "tp", None),
            P("ep", None),
        ),
        out_specs=P("ep", None),
        check_vma=False,
    )
```
